32 devices in a mesh: grp: 2 (over y), bn: 16 (over z, x, core).
Axes of the slice: x: 2, y: 2, z: 4, core: 2. Of those that a mesh axis runs over, the one named last changes fastest.
Arguments:
- images: bfloat16 [32, 19, 19, 384], P(('grp', 'bn')), parts along dimension 0, may hold values from -56 to 56
- expand_weight: bfloat16 [384, 2304], P('bn'), may hold values from -0.3125 to 0.3125
- expand_gain: float32 [2304], replicated, may hold values from 0.5 to 2
- expand_shift: float32 [2304], replicated, may hold values from -3 to 3
- depth_weight: bfloat16 [25, 2304], replicated, may hold values from -1.25 to 1.25
- depth_gain: float32 [2304], replicated, may hold values from 0.5 to 2
- depth_shift: float32 [2304], replicated, may hold values from -3 to 3
- squeeze_weight: bfloat16 [2304, 96], replicated, may hold values from -0.125 to 0.125
- squeeze_bias: float32 [96], replicated, may hold values from -4 to 4
- excite_weight: bfloat16 [96, 2304], replicated, may hold values from -0.625 to 0.625
- excite_bias: float32 [2304], replicated, may hold values from -4 to 4
- project_weight: bfloat16 [2304, 384], P('bn'), may hold values from -0.125 to 0.125
- project_gain: float32 [384], replicated, may hold values from 0.5 to 2
- project_shift: float32 [384], replicated, may hold values from -3 to 3
- group_table: int32 [32], P('grp'), parts along dimension 0, may hold values from 0 to 1, as said below
Outputs:
- block_output: bfloat16 [32, 19, 19, 384], P(('grp', 'bn')), parts along dimension 0
The draws below stay inside these ranges and needn't reach their ends.
There are 2 independent parts, one for each index of `grp`. The reference program is written for one: setup_inputs(seed, part) draws one part's arguments, and reference() takes and returns one part's arrays. A program takes and returns all parts, laid end to end along the dimension named above; an argument that names none is the same for every part. Nothing has to cross between parts.
Inputs may be any that keep to these rules, and one draw needn't show every extreme that they name: `group_table`: each of the 2 statistics groups holds at least 4 images, placed anywhere among the images.
All inputs are finite; a program needn't handle non-finite values.
Results may differ from the reference program's by a relative error of at most 0.0065.
Values may be sent and summed in bfloat16 or wider, within the bound.
A program may use at most 64 MiB of HBM per device.

```python
import math
import jax
import jax.numpy as jnp
from jax import lax

C = 384
EXP = 2304
SQUEEZE = 96
KERNEL = 5
STAT_GROUPS = 2
H = 19
W = 19
IMAGES = 16


def shared_field(key):
    base = jnp.clip(jax.random.normal(key, (IMAGES, H, W), jnp.float32), -4.0, 4.0)
    padded = jnp.pad(base, ((0, 0), (1, 1), (1, 1)))
    total = jnp.zeros((IMAGES, H, W), jnp.float32)
    for row_shift in range(3):
        for col_shift in range(3):
            total = total + padded[:, row_shift:row_shift + H, col_shift:col_shift + W]
    field = jnp.clip(total / 3.0, -2.5, 2.5)
    return (field + 0.4 * (field * field - 1.0)) / 1.15


def draw_images(key, part):
    noise_key = jax.random.fold_in(key, 101)
    offset_key = jax.random.fold_in(key, 102)
    scale_key = jax.random.fold_in(key, 103)
    field_key = jax.random.fold_in(key, 106)
    loading_key = jax.random.fold_in(key, 107)
    loading_sign_key = jax.random.fold_in(key, 108)
    ranks = jnp.arange(IMAGES, dtype=jnp.float32) / max(IMAGES - 1, 1)
    noise = jnp.clip(jax.random.normal(noise_key, (IMAGES, H, W, C), jnp.float32), -4.0, 4.0)
    image_scale = jnp.power(3.0, ranks)
    channel_scale = jnp.exp(jax.random.uniform(scale_key, (1, C), jnp.float32, math.log(0.3), math.log(3.0)))
    loading_signs = jax.random.randint(loading_sign_key, (C,), 0, 2).astype(jnp.float32) * 2.0 - 1.0
    loading = loading_signs * jax.random.uniform(loading_key, (C,), jnp.float32, 0.6, 1.0)
    field = shared_field(field_key)
    noise = noise + 0.9 * field[:, :, :, None] * loading[None, None, None, :]
    offset = 0.5 * jnp.clip(jax.random.normal(offset_key, (IMAGES, C), jnp.float32), -2.0, 2.0)
    scales = channel_scale * image_scale[:, None]
    values = (noise + offset[:, None, None, :]) * scales[:, None, None, :]
    return jnp.clip(values, -56.0, 56.0).astype(jnp.bfloat16)


def draw_group_table(key, part):
    ordering = jax.random.permutation(jax.random.fold_in(key, 201), IMAGES)
    reach = IMAGES // (4 * STAT_GROUPS)
    shifts = jax.random.randint(jax.random.fold_in(key, 202), (STAT_GROUPS - 1,), -reach, reach + 1)
    cuts = jnp.arange(1, STAT_GROUPS, dtype=jnp.int32) * (IMAGES // STAT_GROUPS) + shifts.astype(jnp.int32)
    slots = jnp.arange(IMAGES, dtype=jnp.int32)
    in_order = jnp.sum((slots[:, None] >= cuts[None, :]).astype(jnp.int32), axis=1)
    return in_order[jnp.argsort(ordering)].astype(jnp.int32)


def shard_levels(key, dims, pieces, least, largest):
    def one(dim, blocks):
        heights = jax.random.uniform(jax.random.fold_in(jax.random.fold_in(key, 6), dim), (blocks,), jnp.float32, least / len(pieces), largest / len(pieces))
        return jnp.repeat(jnp.exp(heights), dims[dim] // blocks).reshape((-1,) + (1,) * (len(dims) - dim - 1))

    level = one(*pieces[0])
    for cut in pieces[1:]:
        level = level * one(*cut)
    return level


def normal_values(own_key, extent, spread, most, shards=(), kind=jnp.bfloat16):
    loudness = shard_levels(own_key, extent, shards, -0.22, 0.18) if shards else 1.0
    result = jax.random.normal(own_key, extent, jnp.float32) * spread * loudness
    return jnp.minimum(jnp.maximum(result, -most), most).astype(kind)


def setup_inputs(seed: int = 0, part: int = 0) -> dict:
    key_list = jax.random.split(jax.random.key(seed), 16)
    part_splits = jax.random.split(jax.random.fold_in(key_list[15], part), 16)
    return {
        "images": draw_images(jax.random.fold_in(jax.random.fold_in(key_list[15], part), 71), part),
        "expand_weight": normal_values(key_list[1], (C, EXP), C ** -0.5, 0.3125, ((0, 16),)),
        "expand_gain": jnp.clip(jax.random.uniform(key_list[2], (EXP,), jnp.float32, 0.5, 2.0), 0.5, 2.0),
        "expand_shift": normal_values(key_list[3], (EXP,), 0.5, 3.0, (), jnp.float32),
        "depth_weight": normal_values(key_list[4], (KERNEL * KERNEL, EXP), (KERNEL * KERNEL) ** -0.5, 1.25),
        "depth_gain": jnp.clip(jax.random.uniform(key_list[5], (EXP,), jnp.float32, 0.5, 2.0), 0.5, 2.0),
        "depth_shift": normal_values(key_list[6], (EXP,), 0.5, 3.0, (), jnp.float32),
        "squeeze_weight": normal_values(key_list[7], (EXP, SQUEEZE), EXP ** -0.5, 0.125),
        "squeeze_bias": normal_values(key_list[8], (SQUEEZE,), 1.0, 4.0, (), jnp.float32),
        "excite_weight": normal_values(key_list[9], (SQUEEZE, EXP), SQUEEZE ** -0.5, 0.625),
        "excite_bias": normal_values(key_list[10], (EXP,), 1.0, 4.0, (), jnp.float32),
        "project_weight": normal_values(key_list[11], (EXP, C), EXP ** -0.5, 0.125, ((0, 16),)),
        "project_gain": jnp.clip(jax.random.uniform(key_list[12], (C,), jnp.float32, 0.5, 2.0), 0.5, 2.0),
        "project_shift": normal_values(key_list[13], (C,), 0.5, 3.0, (), jnp.float32),
        "group_table": draw_group_table(jax.random.fold_in(jax.random.fold_in(key_list[15], part), 71), part),
    }


epsilon = 0.001

def normalize(values, centre, inverse, gain, shift):
    return (values.astype(jnp.float32) - centre) * inverse * gain + shift

def depthwise(widened, depth_weight, height, breadth):
    spatial = widened.reshape(height, breadth, widened.shape[-1])
    margin = KERNEL // 2
    padded = jnp.pad(spatial, ((margin, margin), (margin, margin), (0, 0)))
    accumulated = jnp.zeros(spatial.shape, jnp.float32)
    for row_shift in range(KERNEL):
        for col_shift in range(KERNEL):
            window = padded[row_shift:row_shift + height, col_shift:col_shift + breadth]
            accumulated = accumulated + window.astype(jnp.float32) * depth_weight[row_shift * KERNEL + col_shift].astype(jnp.float32)
    return accumulated.reshape(height * breadth, spatial.shape[-1]).astype(jnp.bfloat16)

def group_moments(values, member_table, population):
    totals = lax.optimization_barrier(jnp.sum(values, axis=1, dtype=jnp.float32))
    group_totals = jnp.dot(member_table.T, totals, precision=lax.Precision.HIGHEST)
    centre = jnp.dot(member_table, group_totals / population[:, None], precision=lax.Precision.HIGHEST)

    def centred_squares(bundle):
        return lax.optimization_barrier(jnp.sum(jnp.square(bundle[0].astype(jnp.float32) - bundle[1]), axis=0))
    squares = lax.map(centred_squares, (values, centre))
    group_squares = jnp.dot(member_table.T, squares, precision=lax.Precision.HIGHEST)
    inverse = jnp.dot(member_table, lax.rsqrt(group_squares / population[:, None] + epsilon), precision=lax.Precision.HIGHEST)
    return (centre, inverse)

def reference(images, expand_weight, expand_gain, expand_shift, depth_weight, depth_gain, depth_shift, squeeze_weight, squeeze_bias, excite_weight, excite_bias, project_weight, project_gain, project_shift, group_table):
    pixels = H * W
    flattened = images.reshape(IMAGES, pixels, C)
    labels = jnp.arange(STAT_GROUPS, dtype=jnp.int32)
    member_table = (group_table.astype(jnp.int32)[:, None] == labels[None, :]).astype(jnp.float32)
    population = lax.optimization_barrier(jnp.sum(member_table, axis=0)) * pixels

    def expand_image(picture):
        return jnp.dot(picture, expand_weight, preferred_element_type=jnp.float32).astype(jnp.bfloat16)
    expanded = lax.map(expand_image, flattened)
    centre, inverse = group_moments(expanded, member_table, population)

    def filter_image(bundle):
        widened = jax.nn.silu(normalize(bundle[0], bundle[1], bundle[2], expand_gain, expand_shift)).astype(jnp.bfloat16)
        return depthwise(widened, depth_weight, H, W)
    filtered = lax.map(filter_image, (expanded, centre, inverse))
    centre, inverse = group_moments(filtered, member_table, population)

    def activate_image(bundle):
        return jax.nn.silu(normalize(bundle[0], bundle[1], bundle[2], depth_gain, depth_shift)).astype(jnp.bfloat16)
    activated = lax.map(activate_image, (filtered, centre, inverse))
    pooled = (lax.optimization_barrier(jnp.sum(activated, axis=1, dtype=jnp.float32)) / pixels).astype(jnp.bfloat16)
    squeezed = jax.nn.silu(jnp.dot(pooled, squeeze_weight, preferred_element_type=jnp.float32) + squeeze_bias).astype(jnp.bfloat16)
    excitation = jax.nn.sigmoid(jnp.dot(squeezed, excite_weight, preferred_element_type=jnp.float32) + excite_bias)

    def project_image(bundle):
        gated_input = (bundle[0] * bundle[1]).astype(jnp.bfloat16)
        return jnp.dot(gated_input, project_weight, preferred_element_type=jnp.float32).astype(jnp.bfloat16)
    projected = lax.map(project_image, (activated, excitation))
    centre, inverse = group_moments(projected, member_table, population)
    output = flattened.astype(jnp.float32) + normalize(projected, centre[:, None, :], inverse[:, None, :], project_gain, project_shift)
    return output.astype(jnp.bfloat16).reshape(IMAGES, H, W, C)
```

```python
import functools

import jax
import jax.numpy as jnp
from jax import lax
from jax.experimental import pallas as pl
from jax.experimental.pallas import tpu as pltpu
from jax.sharding import PartitionSpec as P

KERNEL = 5
LANES = 128
MARGIN = KERNEL // 2
epsilon = 0.001
MESH = pl.DeviceIdType.MESH


def silu(v):
    h = 0.5 * v
    return h + h * jnp.tanh(h)


def gather_steps(n, buf, send_sem, recv_sem, rows):
    outer = n // 4
    me = lax.axis_index("bn")
    a, b, c = me // 4, (me // 2) % 2, me % 2

    def index(i, j, k):
        return (i % outer) * 4 + j * 2 + k

    sends = []

    def copy(slot, target, number):
        return pltpu.make_async_remote_copy(
            src_ref=buf.at[slot, pl.ds(0, rows)],
            dst_ref=buf.at[slot, pl.ds(0, rows)],
            send_sem=send_sem.at[number],
            recv_sem=recv_sem.at[slot],
            device_id={"bn": target},
            device_id_type=MESH,
        )

    def send(slot, target):
        move = copy(slot, target, len(sends))
        move.start()
        sends.append(move)

    def await_slot(slot):
        copy(slot, me, 0).wait_recv()

    across, partner = index(a, 1 - b, c), index(a, b, 1 - c)

    def first():
        for d in range(1, outer):
            send(me, index(a + d, b, c))
        send(me, across)
        send(me, partner)

    def second():
        for d in range(1, outer):
            slot = index(a + outer - d, b, c)
            await_slot(slot)
            send(slot, across)
            send(slot, partner)
        await_slot(across)
        send(across, partner)

    def third():
        for d in range(1, outer):
            slot = index(a + outer - d, 1 - b, c)
            await_slot(slot)
            send(slot, partner)
        for i in range(outer):
            for j in range(2):
                await_slot(index(i, j, 1 - c))

    def finish():
        for move in sends:
            move.wait_send()

    return first, second, third, finish


def kernel(
    n, inside, height, breadth, pitch, groups,
    sel_ref, x_ref, w1_ref, g1_ref, s1_ref, dw_ref, g2_ref, s2_ref,
    sqw_ref, sqb_ref, exw_ref, exb_ref, w2_ref, g3_ref, s3_ref,
    out_ref,
    xp, w1, w2, expanded, filtered, wide, narrow, coef, pooled, proj,
    stats, last, w1_send, w1_recv, w2_send, w2_recv, st_send, st_recv,
):
    me = lax.axis_index("bn")
    rows = x_ref.shape[0]
    channels = x_ref.shape[1]
    exp = expanded.shape[1]
    width = exp // groups
    pixels = float(height * breadth)

    def mask_of(lanes):
        column = lax.broadcasted_iota(jnp.int32, (height, pitch, lanes), 1)
        return (column < breadth).reshape(rows, lanes)

    def masked(v):
        lanes = v.shape[1]
        column = lax.broadcasted_iota(jnp.int32, (height, pitch, lanes), 1)
        kept = jnp.where(column < breadth, v.reshape(height, pitch, lanes), 0.0)
        return kept.reshape(rows, lanes)

    def moments(v):
        centre = jnp.sum(v, axis=0, keepdims=True) / pixels
        d = masked(v - centre)
        return jnp.concatenate(
            [centre, jnp.sum(d * d, axis=0, keepdims=True) / pixels], axis=0
        )

    def exchange(e, buf):
        def move(j):
            target = lax.rem(me + j, n)
            return pltpu.make_async_remote_copy(
                src_ref=buf.at[me],
                dst_ref=buf.at[me],
                send_sem=st_send.at[e, j],
                recv_sem=st_recv.at[e, j],
                device_id={"bn": target},
                device_id_type=MESH,
            )

        def start():
            @pl.loop(1, n)
            def _(j):
                move(j).start()

        def wait():
            @pl.loop(1, n)
            def _(j):
                source = lax.rem(me + n - j, n)
                pltpu.make_async_remote_copy(
                    src_ref=buf.at[source],
                    dst_ref=buf.at[source],
                    send_sem=st_send.at[e, j],
                    recv_sem=st_recv.at[e, j],
                    device_id={"bn": me},
                    device_id_type=MESH,
                ).wait_recv()

        def finish():
            @pl.loop(1, n)
            def _(j):
                move(j).wait_send()

        return start, wait, finish

    def combine(buf, gain, shift):
        centre = jnp.zeros(gain.shape, jnp.float32)
        for k in range(n):
            centre = centre + sel_ref[k] * buf[k, 0:1, :]
        spread = jnp.zeros(gain.shape, jnp.float32)
        for k in range(n):
            d = buf[k, 0:1, :] - centre
            spread = spread + sel_ref[k] * (buf[k, 1:2, :] + d * d)
        scale = lax.rsqrt(spread + epsilon) * gain
        return scale, shift - centre * scale

    r1, r2 = w1_ref.shape[0], w2_ref.shape[0]
    if inside:
        slab = w1.shape[1]
        if slab != r1:
            w1[...] = jnp.zeros_like(w1)
        w1[me, 0:r1, :] = w1_ref[...]
        w2[me] = w2_ref[...]
        g1 = gather_steps(n, w1, w1_send, w1_recv, r1)
        g2 = gather_steps(n, w2, w2_send, w2_recv, r2)

    barrier = pltpu.get_barrier_semaphore()

    @pl.loop(1, n)
    def _(j):
        pl.semaphore_signal(
            barrier, inc=1, device_id={"bn": lax.rem(me + j, n)}, device_id_type=MESH
        )

    pl.semaphore_wait(barrier, n - 1)

    if inside:
        g1[0]()
        k = lax.broadcasted_iota(jnp.int32, (channels, n * slab), 0)
        j = lax.broadcasted_iota(jnp.int32, (channels, n * slab), 1)
        bits = slab.bit_length() - 1
        t = jnp.bitwise_and(j, slab - 1)
        target = jnp.right_shift(j, bits) * r1 + t
        spreader = jnp.where((k == target) & (t < r1), 1.0, 0.0).astype(jnp.bfloat16)
        xp[...] = jnp.dot(
            x_ref[...], spreader, preferred_element_type=jnp.float32
        ).astype(jnp.bfloat16)
    wide[...] = jnp.zeros_like(wide)
    if inside:
        g1[1]()
        g1[2]()

    step = 256
    steps = width // step
    first_ex = [exchange(g, stats.at[0, g]) for g in range(groups)]
    second_ex = [exchange(groups + g, stats.at[1, g]) for g in range(groups)]
    third_ex = exchange(2 * groups, last)

    for g in range(groups):
        @pl.loop(0, steps)
        def _(i):
            inner = pl.ds(pl.multiple_of(i * step, step), step)
            cols = pl.ds(pl.multiple_of(g * width + i * step, step), step)
            if inside:
                weights = w1[:, :, cols].reshape(n * slab, step)
                v = jnp.dot(xp[...], weights, preferred_element_type=jnp.float32)
            else:
                v = jnp.dot(x_ref[...], w1_ref[:, cols], preferred_element_type=jnp.float32)
            v = v.astype(jnp.bfloat16)
            expanded[:, cols] = v
            stats[0, g, me, :, inner] = moments(v.astype(jnp.float32))

        first_ex[g][0]()

    if inside:
        g2[0]()

    top = MARGIN * pitch
    small = width // LANES
    for g in range(groups):
        first_ex[g][1]()
        base = pl.ds(g * width, width)
        scale, offset = combine(stats.at[0, g], g1_ref[:, base], s1_ref[:, base])
        coef[0:1, base] = scale
        coef[1:2, base] = offset

        @pl.loop(0, small)
        def _(i):
            inner = pl.ds(pl.multiple_of(i * LANES, LANES), LANES)
            cols = pl.ds(pl.multiple_of(g * width + i * LANES, LANES), LANES)
            v = expanded[:, cols].astype(jnp.float32) * coef[0:1, cols] + coef[1:2, cols]
            wide[pl.ds(top, rows), :] = masked(silu(v))

            def row(y, carry):
                window = [
                    wide[pl.ds(pl.multiple_of((y + r) * pitch, 8), pitch), :]
                    for r in range(KERNEL)
                ]
                total = None
                for s in range(KERNEL):
                    part = None
                    for r in range(KERNEL):
                        tap = r * KERNEL + s
                        term = window[r] * dw_ref[tap : tap + 1, cols]
                        part = term if part is None else part + term
                    turn = (MARGIN - s) % pitch
                    if turn:
                        part = pltpu.roll(part, turn, 0)
                    total = part if total is None else total + part
                narrow[pl.ds(pl.multiple_of(y * pitch, 8), pitch), :] = total
                return carry

            lax.fori_loop(0, height, row, 0, unroll=True)
            f = masked(narrow[...]).astype(jnp.bfloat16)
            filtered[:, cols] = f
            stats[1, g, me, :, inner] = moments(f.astype(jnp.float32))

        second_ex[g][0]()
        if inside and g == groups - 1:
            g2[1]()

    for g in range(groups):
        second_ex[g][1]()
        base = pl.ds(g * width, width)
        scale, offset = combine(stats.at[1, g], g2_ref[:, base], s2_ref[:, base])
        coef[0:1, base] = scale
        coef[1:2, base] = offset

        @pl.loop(0, small)
        def _(i):
            cols = pl.ds(pl.multiple_of(g * width + i * LANES, LANES), LANES)
            v = filtered[:, cols].astype(jnp.float32) * coef[0:1, cols] + coef[1:2, cols]
            v = masked(silu(v))
            filtered[:, cols] = v.astype(jnp.bfloat16)
            pooled[:, cols] = jnp.broadcast_to(
                jnp.sum(v, axis=0, keepdims=True) / pixels, (8, LANES)
            )

    squeezed = silu(
        jnp.dot(
            pooled[...].astype(jnp.bfloat16), sqw_ref[...], preferred_element_type=jnp.float32
        )
        + sqb_ref[...]
    ).astype(jnp.bfloat16)
    gate = (
        jnp.dot(squeezed, exw_ref[...], preferred_element_type=jnp.float32) + exb_ref[...]
    )
    pooled[...] = 0.5 + 0.5 * jnp.tanh(0.5 * gate)

    @pl.loop(0, exp // LANES)
    def _(i):
        cols = pl.ds(pl.multiple_of(i * LANES, LANES), LANES)
        filtered[:, cols] = (
            filtered[:, cols].astype(jnp.float32) * pooled[0:1, cols]
        ).astype(jnp.bfloat16)

    if inside:
        g2[2]()
        weights = w2[...].reshape(n * r2, channels)
    else:
        weights = w2_ref[...]
    proj[...] = jnp.dot(filtered[...], weights, preferred_element_type=jnp.float32)
    last[me] = moments(proj[...])
    third_ex[0]()
    third_ex[1]()
    scale, offset = combine(last, g3_ref[...], s3_ref[...])
    out_ref[...] = (
        x_ref[...].astype(jnp.float32) + (proj[...] * scale + offset)
    ).astype(jnp.bfloat16)

    for e in first_ex + second_ex + [third_ex]:
        e[2]()
    if inside:
        g1[3]()
        g2[3]()


def on_device(
    n, images, expand_weight, expand_gain, expand_shift, depth_weight, depth_gain,
    depth_shift, squeeze_weight, squeeze_bias, excite_weight, excite_bias,
    project_weight, project_gain, project_shift, group_table,
):
    height, breadth, channels = images.shape[1:]
    exp = expand_weight.shape[1]
    pitch = -(-(breadth + MARGIN) // 8) * 8
    rows = height * pitch
    r1, r2 = expand_weight.shape[0], project_weight.shape[0]
    inside = n % 4 == 0 and r1 % 8 == 0 and r2 % 16 == 0
    slab = 16
    while slab < r1:
        slab *= 2
    groups = 3 if exp % (3 * 256) == 0 else 1
    if not inside:
        expand_weight = lax.all_gather(expand_weight, "bn", axis=0, tiled=True)
        project_weight = lax.all_gather(project_weight, "bn", axis=0, tiled=True)
    me = lax.axis_index("bn")
    ranks = jnp.arange(n, dtype=jnp.int32)
    mine = jnp.sum(jnp.where(ranks == me, group_table, 0))
    member = (group_table == mine).astype(jnp.float32)
    sel = member / jnp.sum(member)
    x = jnp.pad(images[0], ((0, 0), (0, pitch - breadth), (0, 0))).reshape(rows, channels)
    f32, bf16 = jnp.float32, jnp.bfloat16
    small = (1, 16, LANES)
    vmem = pl.BlockSpec(memory_space=pltpu.VMEM)
    exchanges = 2 * groups + 1
    out = pl.pallas_call(
        functools.partial(kernel, n, inside, height, breadth, pitch, groups),
        out_shape=jax.ShapeDtypeStruct((rows, channels), bf16),
        in_specs=[pl.BlockSpec(memory_space=pltpu.SMEM)] + [vmem] * 14,
        out_specs=vmem,
        scratch_shapes=[
            pltpu.VMEM((rows, n * slab) if inside else (16, LANES), bf16),
            pltpu.VMEM((n, slab, exp) if inside else small, bf16),
            pltpu.VMEM((n, r2, channels) if inside else small, bf16),
            pltpu.VMEM((rows, exp), bf16),
            pltpu.VMEM((rows, exp), bf16),
            pltpu.VMEM((rows + 2 * MARGIN * pitch, LANES), f32),
            pltpu.VMEM((rows, LANES), f32),
            pltpu.VMEM((2, exp), f32),
            pltpu.VMEM((8, exp), f32),
            pltpu.VMEM((rows, channels), f32),
            pltpu.VMEM((2, groups, n, 2, exp // groups), f32),
            pltpu.VMEM((n, 2, channels), f32),
            pltpu.SemaphoreType.DMA((n,)),
            pltpu.SemaphoreType.DMA((n,)),
            pltpu.SemaphoreType.DMA((n,)),
            pltpu.SemaphoreType.DMA((n,)),
            pltpu.SemaphoreType.DMA((exchanges, n)),
            pltpu.SemaphoreType.DMA((exchanges, n)),
        ],
        compiler_params=pltpu.CompilerParams(
            collective_id=0, has_side_effects=True, vmem_limit_bytes=60 * 1024 * 1024
        ),
    )(
        sel, x, expand_weight, expand_gain[None], expand_shift[None],
        depth_weight.astype(f32), depth_gain[None], depth_shift[None],
        squeeze_weight, squeeze_bias[None], excite_weight, excite_bias[None],
        project_weight, project_gain[None], project_shift[None],
    )
    return out.reshape(height, pitch, channels)[None, :, :breadth]


def solution(mesh):
    n = mesh.shape["bn"]
    return jax.shard_map(
        functools.partial(on_device, n),
        mesh=mesh,
        in_specs=(
            P(("grp", "bn"), None, None, None),
            P("bn", None),
            P(), P(), P(), P(), P(), P(), P(), P(), P(),
            P("bn", None),
            P(), P(),
            P("grp"),
        ),
        out_specs=P(("grp", "bn"), None, None, None),
        check_vma=False,
    )
```

```python
import functools

import jax
import jax.numpy as jnp
from jax import lax
from jax.experimental import pallas as pl
from jax.experimental.pallas import tpu as pltpu
from jax.sharding import PartitionSpec as P

KERNEL = 5
LANES = 128
MARGIN = KERNEL // 2
epsilon = 0.001
MESH = pl.DeviceIdType.MESH


def silu(v):
    h = 0.5 * v
    return h + h * jnp.tanh(h)


def gather_steps(n, buf, send_sem, recv_sem, rows):
    outer = n // 4
    me = lax.axis_index("bn")
    a, b, c = me // 4, (me // 2) % 2, me % 2

    def index(i, j, k):
        return (i % outer) * 4 + j * 2 + k

    sends = []

    def copy(slot, target, number):
        return pltpu.make_async_remote_copy(
            src_ref=buf.at[slot, pl.ds(0, rows)],
            dst_ref=buf.at[slot, pl.ds(0, rows)],
            send_sem=send_sem.at[number],
            recv_sem=recv_sem.at[slot],
            device_id={"bn": target},
            device_id_type=MESH,
        )

    def send(slot, target):
        move = copy(slot, target, len(sends))
        move.start()
        sends.append(move)

    def await_slot(slot):
        copy(slot, me, 0).wait_recv()

    across, partner = index(a, 1 - b, c), index(a, b, 1 - c)

    def first():
        for d in range(1, outer):
            send(me, index(a + d, b, c))
        send(me, across)
        send(me, partner)

    def second():
        for d in range(1, outer):
            slot = index(a + outer - d, b, c)
            await_slot(slot)
            send(slot, across)
            send(slot, partner)
        await_slot(across)
        send(across, partner)

    def third():
        for d in range(1, outer):
            slot = index(a + outer - d, 1 - b, c)
            await_slot(slot)
            send(slot, partner)

    def fourth():
        for i in range(outer):
            for j in range(2):
                await_slot(index(i, j, 1 - c))

    def finish():
        for move in sends:
            move.wait_send()

    return first, second, third, fourth, finish


def kernel(
    n, inside, height, breadth, pitch, groups,
    table_ref, x_ref, w1_ref, dw_ref, g1_ref, s1_ref, g2_ref, s2_ref, exb_ref, g3_ref, s3_ref, sqw_ref, sqb_ref, exw_ref, w2_ref,
    out_ref,
    vec_ref, xp, w1, w2, taps, expanded, filtered, wide, narrow, coef, pooled, proj,
    stats, last, w1_send, w1_recv, w2_send, w2_recv, st_send, st_recv,
):
    me = lax.axis_index("bn")
    rows = x_ref.shape[0]
    channels = x_ref.shape[1]
    exp = expanded.shape[1]
    width = exp // groups
    pixels = float(height * breadth)

    mine = table_ref[me]
    member = [jnp.where(table_ref[k] == mine, 1.0, 0.0) for k in range(n)]
    members = sum(member[1:], member[0])

    def masked(v):
        lanes = v.shape[1]
        column = lax.broadcasted_iota(jnp.int32, (height, pitch, lanes), 1)
        kept = jnp.where(column < breadth, v.reshape(height, pitch, lanes), 0.0)
        return kept.reshape(rows, lanes)

    def moments(v):
        centre = jnp.sum(v, axis=0, keepdims=True) / pixels
        d = masked(v - centre)
        return jnp.concatenate(
            [centre, jnp.sum(d * d, axis=0, keepdims=True) / pixels], axis=0
        )

    def exchange(e, buf):
        def move(j):
            target = lax.rem(me + j, n)
            return pltpu.make_async_remote_copy(
                src_ref=buf.at[me],
                dst_ref=buf.at[me],
                send_sem=st_send.at[e, j],
                recv_sem=st_recv.at[e, j],
                device_id={"bn": target},
                device_id_type=MESH,
            )

        def start():
            @pl.loop(1, n)
            def _(j):
                move(j).start()

        def wait():
            @pl.loop(1, n)
            def _(j):
                source = lax.rem(me + n - j, n)
                pltpu.make_async_remote_copy(
                    src_ref=buf.at[source],
                    dst_ref=buf.at[source],
                    send_sem=st_send.at[e, j],
                    recv_sem=st_recv.at[e, j],
                    device_id={"bn": me},
                    device_id_type=MESH,
                ).wait_recv()

        def finish():
            @pl.loop(1, n)
            def _(j):
                move(j).wait_send()

        return start, wait, finish

    def combine(buf, gain, shift):
        centre = jnp.zeros(gain.shape, jnp.float32)
        for k in range(n):
            centre = centre + member[k] * buf[k, 0:1, :]
        share = 1.0 / jnp.full(gain.shape, members, jnp.float32)
        centre = centre * share
        spread = jnp.zeros(gain.shape, jnp.float32)
        for k in range(n):
            d = buf[k, 0:1, :] - centre
            spread = spread + member[k] * (buf[k, 1:2, :] + d * d)
        scale = lax.rsqrt(spread * share + epsilon) * gain
        return scale, shift - centre * scale

    r1, r2 = w1_ref.shape[0], w2_ref.shape[0]
    if inside:
        slab = w1.shape[1]
        if slab != r1:
            w1[...] = jnp.zeros_like(w1)
        w1[me, 0:r1, :] = w1_ref[...]
        w2[me] = w2_ref[...]
        g1 = gather_steps(n, w1, w1_send, w1_recv, r1)
        g2 = gather_steps(n, w2, w2_send, w2_recv, r2)

    barrier = pltpu.get_barrier_semaphore()

    @pl.loop(1, n)
    def _(j):
        pl.semaphore_signal(
            barrier, inc=1, device_id={"bn": lax.rem(me + j, n)}, device_id_type=MESH
        )

    pl.semaphore_wait(barrier, n - 1)

    if inside:
        g1[0]()
        k = lax.broadcasted_iota(jnp.int32, (channels, n * slab), 0)
        j = lax.broadcasted_iota(jnp.int32, (channels, n * slab), 1)
        bits = slab.bit_length() - 1
        t = jnp.bitwise_and(j, slab - 1)
        target = jnp.right_shift(j, bits) * r1 + t
        spreader = jnp.where((k == target) & (t < r1), 1.0, 0.0).astype(jnp.bfloat16)
        xp[...] = jnp.dot(
            x_ref[...], spreader, preferred_element_type=jnp.float32
        ).astype(jnp.bfloat16)
    wide[...] = jnp.zeros_like(wide)
    taps[...] = dw_ref[...].astype(jnp.float32)
    for k, ref in enumerate((g1_ref, s1_ref, g2_ref, s2_ref, exb_ref, g3_ref, s3_ref)):
        size = ref.shape[0]
        vec_ref[k : k + 1, 0:size] = ref[...].reshape(1, size)
    if inside:
        g1[1]()
        g1[2]()
        g1[3]()

    step = 256
    steps = width // step
    first_ex = [exchange(g, stats.at[0, g]) for g in range(groups)]
    second_ex = [exchange(groups + g, stats.at[1, g]) for g in range(groups)]
    third_ex = exchange(2 * groups, last)

    for g in range(groups):
        @pl.loop(0, steps)
        def _(i):
            inner = pl.ds(pl.multiple_of(i * step, step), step)
            cols = pl.ds(pl.multiple_of(g * width + i * step, step), step)
            if inside:
                weights = w1[:, :, cols].reshape(n * slab, step)
                v = jnp.dot(xp[...], weights, preferred_element_type=jnp.float32)
            else:
                v = jnp.dot(x_ref[...], w1_ref[:, cols], preferred_element_type=jnp.float32)
            v = v.astype(jnp.bfloat16)
            expanded[:, cols] = v
            stats[0, g, me, :, inner] = moments(v.astype(jnp.float32))

        first_ex[g][0]()

    if inside:
        g2[0]()

    top = MARGIN * pitch
    small = width // LANES
    for g in range(groups):
        first_ex[g][1]()
        base = pl.ds(g * width, width)
        scale, offset = combine(stats.at[0, g], vec_ref[0:1, base], vec_ref[1:2, base])
        coef[0:1, base] = scale
        coef[1:2, base] = offset

        @pl.loop(0, small)
        def _(i):
            inner = pl.ds(pl.multiple_of(i * LANES, LANES), LANES)
            cols = pl.ds(pl.multiple_of(g * width + i * LANES, LANES), LANES)
            v = expanded[:, cols].astype(jnp.float32) * coef[0:1, cols] + coef[1:2, cols]
            wide[pl.ds(top, rows), :] = masked(silu(v))

            def row(y, carry):
                window = [
                    wide[pl.ds(pl.multiple_of((y + r) * pitch, 8), pitch), :]
                    for r in range(KERNEL)
                ]
                total = None
                for s in range(KERNEL):
                    part = None
                    for r in range(KERNEL):
                        tap = r * KERNEL + s
                        term = window[r] * taps[tap : tap + 1, cols]
                        part = term if part is None else part + term
                    turn = (MARGIN - s) % pitch
                    if turn:
                        part = pltpu.roll(part, turn, 0)
                    total = part if total is None else total + part
                narrow[pl.ds(pl.multiple_of(y * pitch, 8), pitch), :] = total
                return carry

            lax.fori_loop(0, height, row, 0, unroll=True)
            f = masked(narrow[...]).astype(jnp.bfloat16)
            filtered[:, cols] = f
            stats[1, g, me, :, inner] = moments(f.astype(jnp.float32))

        second_ex[g][0]()
        if inside and g == groups // 2:
            g2[1]()

    for g in range(groups):
        second_ex[g][1]()
        base = pl.ds(g * width, width)
        if inside and g == 0:
            g2[2]()
        scale, offset = combine(stats.at[1, g], vec_ref[2:3, base], vec_ref[3:4, base])
        coef[0:1, base] = scale
        coef[1:2, base] = offset

        @pl.loop(0, small)
        def _(i):
            cols = pl.ds(pl.multiple_of(g * width + i * LANES, LANES), LANES)
            v = filtered[:, cols].astype(jnp.float32) * coef[0:1, cols] + coef[1:2, cols]
            v = masked(silu(v))
            filtered[:, cols] = v.astype(jnp.bfloat16)
            pooled[:, cols] = jnp.broadcast_to(
                jnp.sum(v, axis=0, keepdims=True) / pixels, (8, LANES)
            )

    squeezed = silu(
        lax.dot_general(
            pooled[...].astype(jnp.bfloat16),
            sqw_ref[...],
            (((1,), (1,)), ((), ())),
            preferred_element_type=jnp.float32,
        )
        + sqb_ref[...]
    ).astype(jnp.bfloat16)
    gate = (
        jnp.dot(squeezed, exw_ref[...], preferred_element_type=jnp.float32) + vec_ref[4:5, :]
    )
    pooled[...] = 0.5 + 0.5 * jnp.tanh(0.5 * gate)

    @pl.loop(0, exp // LANES)
    def _(i):
        cols = pl.ds(pl.multiple_of(i * LANES, LANES), LANES)
        filtered[:, cols] = (
            filtered[:, cols].astype(jnp.float32) * pooled[0:1, cols]
        ).astype(jnp.bfloat16)

    if inside:
        g2[3]()
        weights = w2[...].reshape(n * r2, channels)
    else:
        weights = w2_ref[...]
    proj[...] = jnp.dot(filtered[...], weights, preferred_element_type=jnp.float32)
    last[me] = moments(proj[...])
    third_ex[0]()
    third_ex[1]()
    scale, offset = combine(last, vec_ref[5:6, 0:channels], vec_ref[6:7, 0:channels])
    out_ref[...] = (
        x_ref[...].astype(jnp.float32) + (proj[...] * scale + offset)
    ).astype(jnp.bfloat16)

    for e in first_ex + second_ex + [third_ex]:
        e[2]()
    if inside:
        g1[4]()
        g2[4]()


def on_device(
    n, images, expand_weight, expand_gain, expand_shift, depth_weight, depth_gain,
    depth_shift, squeeze_weight, squeeze_bias, excite_weight, excite_bias,
    project_weight, project_gain, project_shift, group_table,
):
    height, breadth, channels = images.shape[1:]
    exp = expand_weight.shape[1]
    pitch = -(-(breadth + MARGIN) // 8) * 8
    rows = height * pitch
    r1, r2 = expand_weight.shape[0], project_weight.shape[0]
    inside = n % 4 == 0 and r1 % 8 == 0 and r2 % 16 == 0
    slab = 16
    while slab < r1:
        slab *= 2
    groups = 3 if exp % (3 * 256) == 0 else 1
    if not inside:
        expand_weight = lax.all_gather(expand_weight, "bn", axis=0, tiled=True)
        project_weight = lax.all_gather(project_weight, "bn", axis=0, tiled=True)
    x = jnp.pad(images[0], ((0, 0), (0, pitch - breadth), (0, 0))).reshape(rows, channels)
    f32, bf16 = jnp.float32, jnp.bfloat16
    small = (1, 16, LANES)
    vmem = pl.BlockSpec(memory_space=pltpu.VMEM)
    exchanges = 2 * groups + 1
    out = pl.pallas_call(
        functools.partial(kernel, n, inside, height, breadth, pitch, groups),
        out_shape=jax.ShapeDtypeStruct((rows, channels), bf16),
        in_specs=[pl.BlockSpec(memory_space=pltpu.SMEM)] + [vmem] * 14,
        out_specs=vmem,
        scratch_shapes=[
            pltpu.VMEM((8, exp), f32),
            pltpu.VMEM((rows, n * slab) if inside else (16, LANES), bf16),
            pltpu.VMEM((n, slab, exp) if inside else small, bf16),
            pltpu.VMEM((n, r2, channels) if inside else small, bf16),
            pltpu.VMEM(depth_weight.shape, f32),
            pltpu.VMEM((rows, exp), bf16),
            pltpu.VMEM((rows, exp), bf16),
            pltpu.VMEM((rows + 2 * MARGIN * pitch, LANES), f32),
            pltpu.VMEM((rows, LANES), f32),
            pltpu.VMEM((2, exp), f32),
            pltpu.VMEM((8, exp), f32),
            pltpu.VMEM((rows, channels), f32),
            pltpu.VMEM((2, groups, n, 2, exp // groups), f32),
            pltpu.VMEM((n, 2, channels), f32),
            pltpu.SemaphoreType.DMA((n,)),
            pltpu.SemaphoreType.DMA((n,)),
            pltpu.SemaphoreType.DMA((n,)),
            pltpu.SemaphoreType.DMA((n,)),
            pltpu.SemaphoreType.DMA((exchanges, n)),
            pltpu.SemaphoreType.DMA((exchanges, n)),
        ],
        compiler_params=pltpu.CompilerParams(
            collective_id=0, has_side_effects=True, vmem_limit_bytes=60 * 1024 * 1024
        ),
    )(
        group_table, x, expand_weight, depth_weight,
        expand_gain, expand_shift, depth_gain, depth_shift, excite_bias,
        project_gain, project_shift,
        squeeze_weight.T, squeeze_bias[None], excite_weight, project_weight,
    )
    return out.reshape(height, pitch, channels)[None, :, :breadth]


def solution(mesh):
    n = mesh.shape["bn"]
    return jax.shard_map(
        functools.partial(on_device, n),
        mesh=mesh,
        in_specs=(
            P(("grp", "bn"), None, None, None),
            P("bn", None),
            P(), P(), P(), P(), P(), P(), P(), P(), P(),
            P("bn", None),
            P(), P(),
            P("grp"),
        ),
        out_specs=P(("grp", "bn"), None, None, None),
        check_vma=False,
    )
```
